32 devices in a mesh: rows: 16 (over z, y, x), cols: 2 (over core).
Axes of the slice: x: 2, y: 2, z: 4, core: 2. Of those that a mesh axis runs over, the one named last changes fastest.
Arguments:
- embeddings: bfloat16 [49152, 1536], P('rows'), may hold values from -43 to 43, as said below
- start_basis: float32 [1536, 256], P(None, 'cols'), may hold values from -6 to 6
Outputs:
- projected: bfloat16 [49152, 256], P('rows', 'cols')
- basis: float32 [1536, 256], P(None, 'cols')
The draws below stay inside these ranges and needn't reach their ends.
Inputs may be any that keep to these rules, and one draw needn't show every extreme that they name: `embeddings`: rows are noisy vectors around offsets that differ between aligned blocks of rows, with per-column spreads that differ by a factor of up to four.
All inputs are finite; a program needn't handle non-finite values.
Results may differ from the reference program's by a relative error of at most 0.025.
Values may be sent and summed in bfloat16 or wider, within the bound.
A program may use at most 64 MiB of HBM per device.

```python
import jax
import jax.numpy as jnp
from jax import lax

D = 1536
K = 256
ROW_DEV = 3072
ITERS = 3
ROWS = 49152


def draw_embeddings(key, part):
    key_offset, key_scale, key_noise = jax.random.split(key, 3)
    key_blocks = jax.random.fold_in(key, 7919)
    offset = jnp.clip(jax.random.normal(key_offset, (D,), jnp.float32), -3.0, 3.0)
    col_scale = jnp.exp(jax.random.uniform(key_scale, (D,), jnp.float32, -0.69, 0.69))
    block_shift = jnp.clip(0.8 * jax.random.normal(key_blocks, (ROWS // ROW_DEV, D), jnp.float32), -3.0, 3.0)
    row_shift = jnp.repeat(block_shift, ROW_DEV, axis=0, total_repeat_length=ROWS)
    noise = jnp.clip(jax.random.normal(key_noise, (ROWS, D), jnp.float32), -5.0, 5.0)
    values = noise * col_scale[None, :] + offset[None, :] + row_shift
    return values.astype(jnp.bfloat16)


def block_scale(rng, extent, pieces, smallest, high):
    def one(dim, blocks):
        steps = jax.random.uniform(jax.random.fold_in(jax.random.fold_in(rng, 6), dim), (blocks,), jnp.float32, smallest / len(pieces), high / len(pieces))
        return jnp.repeat(jnp.exp(steps), extent[dim] // blocks).reshape((-1,) + (1,) * (len(extent) - dim - 1))

    gain = one(*pieces[0])
    for cut in pieces[1:]:
        gain = gain * one(*cut)
    return gain


def normal_values(own_key, shape, width, limit, cuts=(), held_as=jnp.bfloat16):
    values = width * jax.random.normal(own_key, shape, jnp.float32)
    if cuts:
        values = values * block_scale(own_key, shape, cuts, -0.22, 0.18)
    return jnp.clip(values, -limit, limit).astype(held_as)


def setup_inputs(seed: int = 0) -> dict:
    streams_of = jax.random.split(jax.random.key(seed), 3)
    return {
        "embeddings": draw_embeddings(jax.random.fold_in(streams_of[2], 71), 0),
        "start_basis": normal_values(streams_of[1], (D, K), 1.0, 6.0, ((1, 2),), jnp.float32),
    }


def reference(embeddings, start_basis):
    rows_count = embeddings.shape[0]
    col_mean = lax.optimization_barrier(jnp.sum(embeddings, axis=0, dtype=jnp.float32)) / rows_count
    basis = start_basis
    for sweep_index in range(ITERS):
        basis_bf = basis.astype(jnp.bfloat16)
        raw_proj = jnp.dot(embeddings.astype(jnp.float32), basis_bf.astype(jnp.float32), preferred_element_type=jnp.float32)
        offset = jnp.dot(col_mean, basis_bf.astype(jnp.float32), precision=lax.Precision.HIGHEST)
        shifted = (raw_proj - offset[None, :]).astype(jnp.bfloat16)
        col_sums = lax.optimization_barrier(jnp.sum(shifted, axis=0, dtype=jnp.float32))
        products = lax.dot_general(embeddings.astype(jnp.float32), shifted.astype(jnp.float32), (((0,), (0,)), ((), ())), preferred_element_type=jnp.float32)
        products = products - col_mean[:, None] * col_sums[None, :]
        gram_matrix = jnp.dot(products.T, products, precision=lax.Precision.HIGHEST)
        lower = jnp.linalg.cholesky(gram_matrix)
        basis = lax.linalg.triangular_solve(lower, products, left_side=False, lower=True, transpose_a=True)
    centered = embeddings.astype(jnp.float32) - col_mean[None, :]
    unit = (centered * lax.rsqrt(lax.optimization_barrier(jnp.sum(centered * centered, axis=1, keepdims=True)) + 1.0)).astype(jnp.bfloat16)
    coords = jnp.dot(unit.astype(jnp.float32), basis.astype(jnp.bfloat16).astype(jnp.float32), preferred_element_type=jnp.float32)
    scaled = coords * lax.rsqrt(lax.optimization_barrier(jnp.mean(coords * coords, axis=1, keepdims=True)) + 0.0001)
    return (scaled.astype(jnp.bfloat16), basis)
```

```python
import functools

import jax
import jax.numpy as jnp
from jax import lax
from jax.experimental import pallas as pl
from jax.experimental.pallas import tpu as pltpu
from jax.sharding import PartitionSpec as P

ITERS = 3
LANES = 128
MESH = pl.DeviceIdType.MESH
TILES = 4
HI = lax.Precision.HIGHEST
F32 = jnp.float32
BF16 = jnp.bfloat16


def dot(a, b, ca, cb, precision=None):
    return lax.dot_general(a, b, (((ca,), (cb,)), ((), ())), precision=precision, preferred_element_type=F32)


def split(v):
    hi = v.astype(BF16)
    return hi, (v - hi.astype(F32)).astype(BF16)


def inverse_factor(a_ref, spread, k, b):
    w = 2 * b
    lanes = lax.broadcasted_iota(jnp.int32, (b, w), 1)
    subs = lax.broadcasted_iota(jnp.int32, (b, w), 0)
    wide_lane = lax.broadcasted_iota(jnp.int32, (b, k), 1)
    wide_sub = lax.broadcasted_iota(jnp.int32, (b, k), 0)
    sub = lax.broadcasted_iota(jnp.int32, (8, w), 0)
    m = b // 8
    for blk in range(k // b):
        lo, hi = blk * b, (blk + 1) * b
        base = lo % w
        other = b - base
        here = (lanes >= base) & (lanes < base + b)
        first = lo - base
        aug = jnp.where(here, a_ref[lo:hi, first:first + w], (lanes - other == subs).astype(F32))
        tiles = [aug[8 * t:8 * t + 8] for t in range(m)]
        for p in range(m):
            cols = {
                t: [jnp.broadcast_to(tiles[t][:, base + 8 * p + c:base + 8 * p + c + 1], (8, w)) for c in range(8)]
                for t in range(p, m)
            }
            slot = 9 * (p % 2)
            for j in range(8):
                spread[slot + j] = cols[p][j]
            spread[slot + 8] = tiles[p]
            a = [[jnp.broadcast_to(spread[slot + j, i:i + 1, :], (8, w)) for j in range(i + 1)] for i in range(8)]
            low = [jnp.broadcast_to(spread[slot + 8, c:c + 1, :], (8, w)) for c in range(8)]
            inv = []
            for j in range(8):
                r = 1.0 / a[j][j]
                inv.append(r)
                f = {i: a[i][j] * r for i in range(j + 1, 8)}
                for i in range(j + 1, 8):
                    for c in range(j + 1, i + 1):
                        a[i][c] = a[i][c] - f[i] * a[c][j]
                scaled = low[j] * r
                for i in range(j + 1, 8):
                    low[i] = low[i] - f[i] * low[j]
                for t in range(p + 1, m):
                    tiles[t] = tiles[t] - cols[t][j] * scaled
                    for i in range(j + 1, 8):
                        cols[t][i] = cols[t][i] - f[i] * cols[t][j]
            v, d = low[0], inv[0]
            for i in range(1, 8):
                v = jnp.where(sub == i, low[i], v)
                d = jnp.where(sub == i, inv[i], d)
            root = lax.rsqrt(d)
            root = root * (1.5 - 0.5 * d * root * root)
            tiles[p] = v * (d * root)
        factor = jnp.where(here, 0.0, jnp.concatenate(tiles, axis=0))
        inside = (wide_lane >= lo) & (wide_lane < hi)
        rows = jnp.where(inside, (wide_lane - lo == wide_sub).astype(F32), a_ref[lo:hi, :])
        pad = jnp.zeros((b, k), F32)
        strip = dot(factor, jnp.concatenate([pad, rows] if base == 0 else [rows, pad], axis=0), 1, 0, HI)
        for r0 in range(hi, k, b):
            turned = pltpu.roll(a_ref[r0:r0 + b, first:first + w], b, axis=1)
            left = dot(turned, factor, 1, 1, HI)
            old = jnp.where(inside, 0.0, a_ref[r0:r0 + b, :])
            a_ref[r0:r0 + b, :] = old - dot(left, strip, 1, 0, HI)
        a_ref[lo:hi, :] = strip


def finish_kernel(n, total, w_ref, s_ref, b_ref, u_hbm, o_hbm, basis_hbm,
                  w, basis, mean, mean_t, a, spread, unit, out, half, u_sem, o_sem, h_sem):
    core = lax.axis_index("cols")
    d, k = basis.shape
    h = k // 2
    rows = n // TILES

    def unit_copy(i):
        at = pl.ds(pl.multiple_of(i * rows, rows), rows)
        return pltpu.make_async_copy(u_hbm.at[at], unit.at[at], u_sem.at[i])

    for i in range(TILES):
        unit_copy(i).start()
    for (i, l), (c, first, m) in packing(d)[0].items():
        v = w_ref[c, first:first + m, :]
        row, col = i * (d // len(OWNER)), l * LANES
        w[row:row + m, col:col + LANES] = v
        if row + m > col:
            v, m = v[:m - LANES], m - LANES
        if m > 0:
            w[col:col + LANES, row:row + m] = v.T
    s = s_ref[:, 0, :]
    r = s.shape[0]
    m = s * (1.0 / n) - jnp.sum(s, axis=0, keepdims=True) * (1.0 / total)
    mh, ml = split(m)
    mean[:r] = mh
    mean[r:] = ml
    mean_t[...] = jnp.concatenate([mh.astype(F32), ml.astype(F32), mh.astype(F32)], axis=0).T.astype(BF16)
    basis[...] = jnp.concatenate([b_ref[0], b_ref[1]], axis=1)
    cut = d // 2

    @pl.loop(0, ITERS)
    def _(_):
        bf = basis[...]
        inner = dot(mean[...], bf, 1, 0)
        ih, il = split((inner[:r] + inner[r:]) * float(n))
        side = jnp.concatenate([ih, ih, il], axis=0)
        parts = []
        for g in range(2):
            at = slice(g * cut, (g + 1) * cut)
            parts.append(split(dot(w[at, :], bf, 1, 0) + dot(mean_t[at, :], side, 1, 0)))
        hh, cross, ll = 0.0, 0.0, 0.0
        for ph, plo in parts:
            hh += dot(ph, ph, 0, 0)
            cross += dot(plo, ph, 0, 0)
            ll += dot(plo, plo, 0, 0)
        a[...] = hh + (ll + (cross + cross.T))
        inverse_factor(a, spread, k, 64)
        below = lax.broadcasted_iota(jnp.int32, (k, k), 0) >= lax.broadcasted_iota(jnp.int32, (k, k), 1)
        lh, ll = split(jnp.where(below, a[...], 0.0))
        for g, (ph, plo) in enumerate(parts):
            new = dot(ph, lh, 1, 1) + (dot(ph, ll, 1, 1) + dot(plo, lh, 1, 1))
            at = slice(g * cut, (g + 1) * cut)
            half[at, :] = jnp.where(core == 0, new[:, :h], new[:, h:])
            basis[at, :] = new.astype(BF16)

    half_copy = pltpu.make_async_copy(half, basis_hbm, h_sem)
    half_copy.start()

    def out_copy(i):
        at = pl.ds(pl.multiple_of(i * rows, rows), rows)
        return pltpu.make_async_copy(out.at[at], o_hbm.at[at], o_sem.at[i])

    @pl.loop(0, TILES)
    def _(i):
        unit_copy(i).wait()
        for g in range(2):
            at = pl.ds(pl.multiple_of(i * rows + g * (rows // 2), rows // 2), rows // 2)
            coords = dot(unit[at, :], basis[...], 1, 0)
            scale = lax.rsqrt(jnp.sum(coords * coords, axis=1, keepdims=True) * (1.0 / k) + 0.0001)
            out[at, :] = (jnp.where(core == 0, coords[:, :h], coords[:, h:]) * scale).astype(BF16)
        out_copy(i).start()

    half_copy.wait()
    for i in range(TILES):
        out_copy(i).wait()


def finish(n, total, w, s, b, u):
    d, h = b.shape[1], b.shape[2]
    k = 2 * h
    vm = pl.BlockSpec(memory_space=pltpu.VMEM)
    hbm = pl.BlockSpec(memory_space=pl.ANY)
    dma = pltpu.SemaphoreType.DMA
    return pl.pallas_call(
        functools.partial(finish_kernel, n, total),
        in_specs=[vm] * 3 + [hbm],
        out_specs=[hbm] * 2,
        out_shape=[jax.ShapeDtypeStruct((n, h), BF16), jax.ShapeDtypeStruct((d, h), F32)],
        scratch_shapes=[
            pltpu.VMEM((d, d), BF16),
            pltpu.VMEM((d, k), BF16),
            pltpu.VMEM((2 * s.shape[0], d), BF16),
            pltpu.VMEM((d, 3 * s.shape[0]), BF16),
            pltpu.VMEM((k, k), F32),
            pltpu.VMEM((18, 8, LANES), F32),
            pltpu.VMEM((n, d), BF16),
            pltpu.VMEM((n, h), BF16),
            pltpu.VMEM((d, h), F32),
            dma((TILES,)),
            dma((TILES,)),
            dma(()),
        ],
    )(w, s, b, u)


def factors(r):
    z = 4 if r % 4 == 0 else 1
    x = 1
    while x * x < r // z:
        x *= 2
    return z, r // z // x, x


def split3(v):
    hi, rest = split(v)
    rest = v - hi.astype(F32)
    mid = rest.astype(BF16).astype(F32)
    return hi.astype(F32), mid, (rest - mid).astype(BF16).astype(F32)


def stack(parts, order):
    pad = jnp.zeros((16 - len(order), parts[0].shape[1]), F32)
    return jnp.concatenate([parts[i] for i in order] + [pad], axis=0).astype(BF16)


OWNER = (0, 1, 0, 1, 1, 1)
SLOTS = (
    (((0, 0, 3),), ((0, 3, 6),), ((2, 2, 4),), ((2, 4, 6),)),
    (((1, 1, 4),), ((1, 4, 6),), ((3, 3, 6),), ((4, 4, 6), (5, 5, 6))),
)
LAG = 3
UNITS = 12
STEP = 128


def packing(d):
    t = d // len(OWNER)
    firsts, fill = {}, [0, 0]
    for i, c in enumerate(OWNER):
        for l in range(i * t // LANES, d // LANES):
            m = min(t, (l + 1) * LANES - i * t)
            firsts[i, l] = (c, fill[c], m)
            fill[c] += m
    return firsts, fill


def packed_length(d, r):
    unit = 5 * 16 * r
    return -(-max(packing(d)[1]) // unit) * unit


def stream_count(length, r):
    return 10 if length % (160 * r) == 0 else 5


def plans_of(streams):
    return [(("x", "y", "z"), ("y", "x", "z"))[q % 2] for q in range(streams)]


def reduce_kernel(r, e_hbm, b_ref, wout, sout, bout, u_hbm, e, acc, ssum, left, right, w_ref, e_sem, *scratch):
    nz, ny, nx = factors(r)
    n, d = e.shape
    t = d // len(OWNER)
    firsts, fill = packing(d)
    length = w_ref.shape[0]
    streams = stream_count(length, r)
    plans = plans_of(streams)
    size = {"x": nx, "y": ny, "z": nz}
    stride = {"x": 1, "y": nx, "z": nx * ny}
    scratch = list(scratch)
    stage = [[scratch.pop(0) for _ in plan] for plan in plans]
    held = [[scratch.pop(0) for _ in plan[:-1]] for plan in plans]
    w_recv, s_recv, w_send, s_send, c_send, c_recv, b_send, b_recv, u_sem = scratch

    me = lax.axis_index("rows")
    core = lax.axis_index("cols")
    tile = n // TILES

    def tile_copy(i):
        at_rows = pl.ds(pl.multiple_of(i * tile, tile), tile)
        return pltpu.make_async_copy(e_hbm.at[at_rows], e.at[at_rows], e_sem.at[i])

    for i in range(TILES):
        tile_copy(i).start()
    at = {a: lax.rem(me // stride[a], size[a]) for a in size}
    partner = {"cols": 1 - core}

    def peer(a, k):
        p = lax.rem(at[a] + k, size[a])
        return p, {"rows": me + (p - at[a]) * stride[a]}

    barrier = pltpu.get_barrier_semaphore()
    count = 1
    pl.semaphore_signal(barrier, inc=1, device_id=partner, device_id_type=MESH)
    for a in size:
        for k in range(1, size[a]):
            pl.semaphore_signal(barrier, inc=1, device_id=peer(a, k)[1], device_id_type=MESH)
            count += 1
    pl.semaphore_wait(barrier, count)

    def remote(src, dst, send, recv, device):
        pltpu.make_async_remote_copy(
            src_ref=src, dst_ref=dst, send_sem=send, recv_sem=recv, device_id=device, device_id_type=MESH
        ).start()

    def settle(ref, sem):
        pltpu.make_async_copy(ref, ref, sem).wait()

    def rows_of(off, m):
        return pl.ds(pl.multiple_of(off, 16), m)

    off = [q * (length // streams) for q in range(streams)]
    span = [length // streams] * streams

    def start_reduce(q, ph):
        a = plans[q][ph]
        m = span[q] // size[a]
        for k in range(1, size[a]):
            p, dev = peer(a, k)
            src = w_ref.at[rows_of(off[q] + p * m, m)] if ph == 0 else held[q][ph - 1].at[rows_of(p * m, m)]
            remote(src, stage[q][ph].at[k - 1], w_send, w_recv.at[q, ph], dev)

    def finish_reduce(q, ph):
        a = plans[q][ph]
        g = size[a]
        m = span[q] // g
        if g > 1:
            settle(stage[q][ph], w_recv.at[q, ph])
        mine = rows_of(off[q] + at[a] * m, m) if ph == 0 else rows_of(at[a] * m, m)
        total = (w_ref[mine] if ph == 0 else held[q][ph - 1][mine]).astype(F32)
        for k in range(g - 1):
            total = total + stage[q][ph][k].astype(F32)
        off[q] = off[q] + at[a] * m
        span[q] = m
        if ph < len(plans[q]) - 1:
            held[q][ph][...] = total.astype(BF16)
        else:
            wout[core, rows_of(off[q], m)] = total.astype(BF16)

    def start_gather(q, ph):
        a = plans[q][ph]
        block = wout.at[core, rows_of(off[q], span[q])]
        for k in range(1, size[a]):
            remote(block, block, w_send, w_recv.at[q, 3 + ph], peer(a, k)[1])

    def send_across(row, m):
        block = wout.at[core, rows_of(row, m)]
        remote(block, block, c_send, c_recv, partner)

    def finish_gather(q, ph):
        a = plans[q][ph]
        if size[a] > 1:
            settle(stage[q][ph], w_recv.at[q, 3 + ph])
        off[q] = off[q] - at[a] * span[q]
        span[q] = span[q] * size[a]
        if ph == 1:
            send_across(off[q], span[q])
        if ph == 0:
            part = span[q] // size[a]
            for k in range(1, size[a]):
                send_across(off[q] + peer(a, k)[0] * part, part)

    def advance(q, st):
        if st < 3:
            finish_reduce(q, st)
            if st < 2:
                start_reduce(q, st + 1)
            else:
                start_gather(q, 2)
        else:
            finish_gather(q, 5 - st)
            if st < 5:
                start_gather(q, 4 - st)

    def start_sums(ph):
        a = "xyz"[ph]
        width = stride[a]
        block = pl.ds(me // width * width, width)
        for k in range(1, size[a]):
            remote(sout.at[block], sout.at[block], s_send, s_recv.at[ph], peer(a, k)[1])

    def finish_sums(ph):
        a = "xyz"[ph]
        if size[a] > 1:
            settle(sout.at[pl.ds(0, (size[a] - 1) * stride[a])], s_recv.at[ph])

    bout[core] = b_ref[...].astype(BF16)
    remote(bout.at[core], bout.at[core], b_send, b_recv, partner)
    ssum[...] = jnp.zeros_like(ssum)
    started = 0
    ready = [0, 0]
    for slot in range(len(SLOTS[0])):
        for c in range(2):
            @pl.when(core == c)
            def _(slot=slot, c=c):
                work, at_col = [], 0
                for i, lo, hi in SLOTS[c][slot]:
                    work.append((i, lo * t, hi * t, at_col))
                    at_col += (hi - lo) * t
                acc[:, :at_col] = jnp.zeros((t, at_col), F32)
                reps = TILES if slot == 0 else 2
                deep = n // reps

                @pl.loop(0, reps)
                def _(step):
                    if slot == 0:
                        tile_copy(step).wait()
                    part = pl.ds(pl.multiple_of(step * deep, deep), deep)
                    if slot == 0:
                        ssum[...] += dot(jnp.ones((8, deep), BF16), e[part, :], 1, 0)
                    for i, lo, hi, col in work:
                        acc[:, col:col + hi - lo] += dot(e[part, i * t:(i + 1) * t], e[part, lo:hi], 0, 0)

                if slot == 0:
                    sums = ssum[0:1, :]
                    left[...] = stack(split3(sums * (1.0 / n)), (0, 0, 1, 1, 0, 2))
                    right[...] = stack(split3(sums), (0, 1, 0, 1, 2, 0))
                for i, lo, hi, col in work:
                    v = acc[:, col:col + hi - lo] - dot(left[:, i * t:(i + 1) * t], right[:, lo:hi], 0, 0)
                    v = v.astype(BF16)
                    for l in range(lo // LANES, hi // LANES):
                        _, first, m = firsts[i, l]
                        w_ref[first:first + m, :] = v[:m, l * LANES - lo:(l + 1) * LANES - lo]
                if slot == len(SLOTS[0]) - 1 and fill[c] < length:
                    w_ref[fill[c]:length, :] = jnp.zeros((length - fill[c], LANES), BF16)

        for c in range(2):
            for i, lo, hi in SLOTS[c][slot]:
                ready[c] = sum(firsts[i, hi * t // LANES - 1][1:])
        until = streams if slot == len(SLOTS[0]) - 1 else min(ready) * streams // length
        for q in range(started, until):
            start_reduce(q, 0)
        started = until
        if slot == 0:
            sout[me] = ssum[0:1, :]
            start_sums(0)
        elif slot < 3:
            finish_sums(slot - 1)
            start_sums(slot)
    finish_sums(2)
    mean = jnp.sum(sout[:, 0, :], axis=0, keepdims=True) * (1.0 / (n * r))

    def make_unit(i):
        @pl.loop(0, n // UNITS // STEP)
        def _(step):
            at_rows = pl.ds(pl.multiple_of(i * (n // UNITS) + step * STEP, STEP), STEP)
            centered = e[at_rows, :].astype(F32) - mean
            e[at_rows, :] = (
                centered * lax.rsqrt(jnp.sum(centered * centered, axis=1, keepdims=True) + 1.0)
            ).astype(BF16)

        at_rows = pl.ds(i * (n // UNITS), n // UNITS)
        pltpu.make_async_copy(e.at[at_rows], u_hbm.at[at_rows], u_sem).start()

    events = sorted((q + LAG * st, st, q) for q in range(streams) for st in range(6))
    units = 0
    for at_event, (_, st, q) in enumerate(events):
        advance(q, st)
        if at_event % 4 == 1 and units < UNITS:
            make_unit(units)
            units += 1
    while units < UNITS:
        make_unit(units)
        units += 1
    settle(wout.at[0], c_recv)
    settle(wout.at[0], c_send)
    settle(bout.at[0], b_recv)
    settle(bout.at[0], b_send)
    settle(wout.at[:, pl.ds(0, length - length // r)], w_send)
    settle(sout.at[pl.ds(0, r - 1)], s_send)
    pltpu.make_async_copy(e, u_hbm, u_sem).wait()


def reduce(r, e, b):
    n, d = e.shape
    t = d // len(OWNER)
    length = packed_length(d, r)
    nz, ny, nx = factors(r)
    size = {"x": nx, "y": ny, "z": nz}
    streams = stream_count(length, r)
    stages, helds = [], []
    for plan in plans_of(streams):
        m = length // streams
        for ph, a in enumerate(plan):
            m //= size[a]
            stages.append(pltpu.VMEM((max(size[a] - 1, 1), m, LANES), BF16))
            if ph < 2:
                helds.append(pltpu.VMEM((m, LANES), BF16))
    vm = pl.BlockSpec(memory_space=pltpu.VMEM)
    hbm = pl.BlockSpec(memory_space=pl.ANY)
    dma = pltpu.SemaphoreType.DMA
    return pl.pallas_call(
        functools.partial(reduce_kernel, r),
        in_specs=[hbm, vm],
        out_specs=[vm] * 3 + [hbm],
        out_shape=[
            jax.ShapeDtypeStruct((2, length, LANES), BF16),
            jax.ShapeDtypeStruct((r, 1, d), F32),
            jax.ShapeDtypeStruct((2,) + b.shape, BF16),
            jax.ShapeDtypeStruct((n, d), BF16),
        ],
        scratch_shapes=[
            pltpu.VMEM((n, d), BF16),
            pltpu.VMEM((t, 3 * t), F32),
            pltpu.VMEM((8, d), F32),
            pltpu.VMEM((16, d), BF16),
            pltpu.VMEM((16, d), BF16),
            pltpu.VMEM((length, LANES), BF16),
            dma((TILES,)),
        ]
        + stages + helds + [dma((streams, 6)), dma((3,))] + [dma(())] * 7,
        compiler_params=pltpu.CompilerParams(collective_id=0, has_side_effects=True),
    )(e, b)


def shards(embeddings, start_basis):
    n, d = embeddings.shape
    r = lax.axis_size("rows")
    w, s, b, u = reduce(r, embeddings, start_basis)
    return finish(n, n * r, w, s, b, u)


def solution(mesh):
    in_specs = (P("rows", None), P(None, "cols"))
    out_specs = (P("rows", "cols"), P(None, "cols"))
    return jax.shard_map(shards, mesh=mesh, in_specs=in_specs, out_specs=out_specs, check_vma=False)
```

```python
import functools

import jax
import jax.numpy as jnp
from jax import lax
from jax.experimental import pallas as pl
from jax.experimental.pallas import tpu as pltpu
from jax.sharding import PartitionSpec as P

ITERS = 3
LANES = 128
MESH = pl.DeviceIdType.MESH
TILES = 4
VMEM = 32 << 20
HI = lax.Precision.HIGHEST
F32 = jnp.float32
BF16 = jnp.bfloat16


def dot(a, b, ca, cb, precision=None):
    return lax.dot_general(a, b, (((ca,), (cb,)), ((), ())), precision=precision, preferred_element_type=F32)


def split(v):
    hi = v.astype(BF16)
    return hi, (v - hi.astype(F32)).astype(BF16)


def inverse_factor(a_ref, spread, k, b):
    w = 2 * b
    lanes = lax.broadcasted_iota(jnp.int32, (b, w), 1)
    subs = lax.broadcasted_iota(jnp.int32, (b, w), 0)
    wide_lane = lax.broadcasted_iota(jnp.int32, (b, k), 1)
    wide_sub = lax.broadcasted_iota(jnp.int32, (b, k), 0)
    sub = lax.broadcasted_iota(jnp.int32, (8, w), 0)
    m = b // 8
    for blk in range(k // b):
        lo, hi = blk * b, (blk + 1) * b
        base = lo % w
        other = b - base
        here = (lanes >= base) & (lanes < base + b)
        first = lo - base
        aug = jnp.where(here, a_ref[lo:hi, first:first + w], (lanes - other == subs).astype(F32))
        tiles = [aug[8 * t:8 * t + 8] for t in range(m)]
        for p in range(m):
            cols = {
                t: [jnp.broadcast_to(tiles[t][:, base + 8 * p + c:base + 8 * p + c + 1], (8, w)) for c in range(8)]
                for t in range(p, m)
            }
            slot = 9 * (p % 2)
            for j in range(8):
                spread[slot + j] = cols[p][j]
            spread[slot + 8] = tiles[p]
            a = [[jnp.broadcast_to(spread[slot + j, i:i + 1, :], (8, w)) for j in range(i + 1)] for i in range(8)]
            low = [jnp.broadcast_to(spread[slot + 8, c:c + 1, :], (8, w)) for c in range(8)]
            inv = []
            for j in range(8):
                r = 1.0 / a[j][j]
                inv.append(r)
                f = {i: a[i][j] * r for i in range(j + 1, 8)}
                for i in range(j + 1, 8):
                    for c in range(j + 1, i + 1):
                        a[i][c] = a[i][c] - f[i] * a[c][j]
                scaled = low[j] * r
                for i in range(j + 1, 8):
                    low[i] = low[i] - f[i] * low[j]
                for t in range(p + 1, m):
                    tiles[t] = tiles[t] - cols[t][j] * scaled
                    for i in range(j + 1, 8):
                        cols[t][i] = cols[t][i] - f[i] * cols[t][j]
            v, d = low[0], inv[0]
            for i in range(1, 8):
                v = jnp.where(sub == i, low[i], v)
                d = jnp.where(sub == i, inv[i], d)
            root = lax.rsqrt(d)
            root = root * (1.5 - 0.5 * d * root * root)
            tiles[p] = v * (d * root)
        factor = jnp.where(here, 0.0, jnp.concatenate(tiles, axis=0))
        inside = (wide_lane >= lo) & (wide_lane < hi)
        rows = jnp.where(inside, (wide_lane - lo == wide_sub).astype(F32), a_ref[lo:hi, :])
        pad = jnp.zeros((b, k), F32)
        strip = dot(factor, jnp.concatenate([pad, rows] if base == 0 else [rows, pad], axis=0), 1, 0, HI)
        for r0 in range(hi, k, b):
            turned = pltpu.roll(a_ref[r0:r0 + b, first:first + w], b, axis=1)
            left = dot(turned, factor, 1, 1, HI)
            old = jnp.where(inside, 0.0, a_ref[r0:r0 + b, :])
            a_ref[r0:r0 + b, :] = old - dot(left, strip, 1, 0, HI)
        a_ref[lo:hi, :] = strip


def finish_kernel(n, total, w_ref, s_ref, b_ref, u_hbm, o_hbm, basis_hbm,
                  w, basis, mean, mean_t, a, spread, unit, out, half, u_sem, o_sem, h_sem):
    core = lax.axis_index("cols")
    d, k = basis.shape
    h = k // 2
    rows = n // TILES

    def unit_copy(i):
        at = pl.ds(pl.multiple_of(i * rows, rows), rows)
        return pltpu.make_async_copy(u_hbm.at[at], unit.at[at], u_sem.at[i])

    for i in range(TILES):
        unit_copy(i).start()
    for (i, l), (c, first, m) in packing(d)[0].items():
        v = w_ref[c, first:first + m, :]
        row, col = i * (d // len(OWNER)), l * LANES
        w[row:row + m, col:col + LANES] = v
        if row + m > col:
            v, m = v[:m - LANES], m - LANES
        if m > 0:
            w[col:col + LANES, row:row + m] = v.T
    s = s_ref[:, 0, :]
    r = s.shape[0]
    m = s * (1.0 / n) - jnp.sum(s, axis=0, keepdims=True) * (1.0 / total)
    mh, ml = split(m)
    mean[:r] = mh
    mean[r:] = ml
    mean_t[...] = jnp.concatenate([mh.astype(F32), ml.astype(F32), mh.astype(F32)], axis=0).T.astype(BF16)
    basis[...] = jnp.concatenate([b_ref[0], b_ref[1]], axis=1)
    cut = d // 2

    @pl.loop(0, ITERS)
    def _(_):
        bf = basis[...]
        inner = dot(mean[...], bf, 1, 0)
        ih, il = split((inner[:r] + inner[r:]) * float(n))
        side = jnp.concatenate([ih, ih, il], axis=0)
        parts = []
        for g in range(2):
            at = slice(g * cut, (g + 1) * cut)
            parts.append(split(dot(w[at, :], bf, 1, 0) + dot(mean_t[at, :], side, 1, 0)))
        for corner in (LANES, k):
            hh, cross, ll = 0.0, 0.0, 0.0
            for ph, plo in parts:
                ph, plo = ph[:, :corner], plo[:, :corner]
                hh += dot(ph, ph, 0, 0)
                cross += dot(plo, ph, 0, 0)
                ll += dot(plo, plo, 0, 0)
            part = hh + (ll + (cross + cross.T))
            if corner < k:
                a[:corner, :corner] = part
            else:
                a[:LANES, LANES:] = part[:LANES, LANES:]
                a[LANES:, :] = part[LANES:, :]
        inverse_factor(a, spread, k, 64)
        below = lax.broadcasted_iota(jnp.int32, (k, k), 0) >= lax.broadcasted_iota(jnp.int32, (k, k), 1)
        lh, ll = split(jnp.where(below, a[...], 0.0))
        for g, (ph, plo) in enumerate(parts):
            new = dot(ph, lh, 1, 1) + (dot(ph, ll, 1, 1) + dot(plo, lh, 1, 1))
            at = slice(g * cut, (g + 1) * cut)
            half[at, :] = jnp.where(core == 0, new[:, :h], new[:, h:])
            basis[at, :] = new.astype(BF16)

    half_copy = pltpu.make_async_copy(half, basis_hbm, h_sem)
    half_copy.start()

    def out_copy(i):
        at = pl.ds(pl.multiple_of(i * rows, rows), rows)
        return pltpu.make_async_copy(out.at[at], o_hbm.at[at], o_sem.at[i])

    @pl.loop(0, TILES)
    def _(i):
        unit_copy(i).wait()
        for g in range(2):
            at = pl.ds(pl.multiple_of(i * rows + g * (rows // 2), rows // 2), rows // 2)
            coords = dot(unit[at, :], basis[...], 1, 0)
            scale = lax.rsqrt(jnp.sum(coords * coords, axis=1, keepdims=True) * (1.0 / k) + 0.0001)
            out[at, :] = (jnp.where(core == 0, coords[:, :h], coords[:, h:]) * scale).astype(BF16)
        out_copy(i).start()

    half_copy.wait()
    for i in range(TILES):
        out_copy(i).wait()


def finish(n, total, w, s, b, u):
    d, h = b.shape[1], b.shape[2]
    k = 2 * h
    vm = pl.BlockSpec(memory_space=pltpu.VMEM)
    hbm = pl.BlockSpec(memory_space=pltpu.HBM)
    dma = pltpu.SemaphoreType.DMA
    return pl.pallas_call(
        functools.partial(finish_kernel, n, total),
        in_specs=[vm] * 3 + [hbm],
        out_specs=[hbm] * 2,
        out_shape=[jax.ShapeDtypeStruct((n, h), BF16), jax.ShapeDtypeStruct((d, h), F32)],
        scratch_shapes=[
            pltpu.VMEM((d, d), BF16),
            pltpu.VMEM((d, k), BF16),
            pltpu.VMEM((2 * s.shape[0], d), BF16),
            pltpu.VMEM((d, 3 * s.shape[0]), BF16),
            pltpu.VMEM((k, k), F32),
            pltpu.VMEM((18, 8, LANES), F32),
            pltpu.VMEM((n, d), BF16),
            pltpu.VMEM((n, h), BF16),
            pltpu.VMEM((d, h), F32),
            dma((TILES,)),
            dma((TILES,)),
            dma(()),
        ],
        compiler_params=pltpu.CompilerParams(vmem_limit_bytes=VMEM),
    )(w, s, b, u)


def factors(r):
    z = 4 if r % 4 == 0 else 1
    x = 1
    while x * x < r // z:
        x *= 2
    return z, r // z // x, x


def split3(v):
    hi, rest = split(v)
    rest = v - hi.astype(F32)
    mid = rest.astype(BF16).astype(F32)
    return hi.astype(F32), mid, (rest - mid).astype(BF16).astype(F32)


def stack(parts, order):
    pad = jnp.zeros((16 - len(order), parts[0].shape[1]), F32)
    return jnp.concatenate([parts[i] for i in order] + [pad], axis=0).astype(BF16)


OWNER = (0, 1, 0, 1, 1, 1)
SLOTS = (
    (((0, 0, 3),), ((0, 3, 6),), ((2, 2, 4),), ((2, 4, 6),)),
    (((1, 1, 4),), ((1, 4, 6),), ((3, 3, 6),), ((4, 4, 6), (5, 5, 6))),
)
UNITS = 12
STEP = 128


def packing(d):
    t = d // len(OWNER)
    firsts, fill = {}, [0, 0]
    for i, c in enumerate(OWNER):
        for l in range(i * t // LANES, d // LANES):
            m = min(t, (l + 1) * LANES - i * t)
            firsts[i, l] = (c, fill[c], m)
            fill[c] += m
    return firsts, fill


def packed_length(d, r):
    unit = 5 * 16 * r
    return -(-max(packing(d)[1]) // unit) * unit


def stream_count(length, r):
    return 10 if length % (160 * r) == 0 else 5


PLANS = ("xyz", "yxz", "xyz", "yxz", "zxy")
SLOT_US = (3.3, 1.2, 1.2, 1.4)
RATE = 87e3
FLIGHT_US = {"x": 2.2, "y": 2.2, "z": 2.9}
STEP_US = 0.2
UNIT_US = 0.5


def plans_of(streams):
    return [PLANS[q % len(PLANS)] for q in range(streams)]


def timetable(streams, plans, size, chunk, until):
    free = dict.fromkeys("xyz", 0.0)
    due, table = {}, []
    now, left = 0.0, UNITS

    def launch(q, st):
        plan = plans[q]
        ph = min(st, 5 - st)
        share = chunk
        for a in plan[:ph + 1]:
            share /= size[a]
        g = size[plan[ph]]
        free[plan[ph]] = max(now, free[plan[ph]]) + share * (g // 2) * (g - g // 2) / RATE
        due[q] = (free[plan[ph]] + FLIGHT_US[plan[ph]], q, st)

    def take(at):
        _, q, st = at
        del due[q]
        if st < 5:
            launch(q, st + 1)
        return st, q

    started = 0
    for cost, stop in zip(SLOT_US, until):
        now += cost
        for q in range(started, stop):
            launch(q, 0)
        started = stop
        step = []
        if stop < streams:
            for at in sorted(v for v in due.values() if v[0] <= now):
                now += STEP_US
                step.append(take(at))
        table.append(step)
    while due:
        at = min(due.values())
        if left and at[0] - now > 0.3:
            now += UNIT_US
            left -= 1
            table[-1].append(None)
        else:
            now = max(now, at[0]) + STEP_US
            table[-1].append(take(at))
    table[-1] += [None] * left
    return table


def reduce_kernel(r, e_hbm, b_ref, wout, sout, bout, u_hbm, e, acc, ssum, left, right, w_ref, e_sem, *scratch):
    nz, ny, nx = factors(r)
    n, d = e.shape
    t = d // len(OWNER)
    firsts, fill = packing(d)
    length = w_ref.shape[0]
    streams = stream_count(length, r)
    plans = plans_of(streams)
    size = {"x": nx, "y": ny, "z": nz}
    stride = {"x": 1, "y": nx, "z": nx * ny}
    scratch = list(scratch)
    stage = [[scratch.pop(0) for _ in plan] for plan in plans]
    held = [[scratch.pop(0) for _ in plan[:-1]] for plan in plans]
    w_recv, s_recv, w_send, s_send, c_send, c_recv, b_send, b_recv, u_sem = scratch

    me = lax.axis_index("rows")
    core = lax.axis_index("cols")
    tile = n // TILES

    def tile_copy(i):
        at_rows = pl.ds(pl.multiple_of(i * tile, tile), tile)
        return pltpu.make_async_copy(e_hbm.at[at_rows], e.at[at_rows], e_sem.at[i])

    for i in range(TILES):
        tile_copy(i).start()
    at = {a: lax.rem(me // stride[a], size[a]) for a in size}
    partner = {"cols": 1 - core}

    def peer(a, k):
        p = lax.rem(at[a] + k, size[a])
        return p, {"rows": me + (p - at[a]) * stride[a]}

    barrier = pltpu.get_barrier_semaphore()
    count = 1
    pl.semaphore_signal(barrier, inc=1, device_id=partner, device_id_type=MESH)
    for a in size:
        for k in range(1, size[a]):
            pl.semaphore_signal(barrier, inc=1, device_id=peer(a, k)[1], device_id_type=MESH)
            count += 1
    pl.semaphore_wait(barrier, count)

    def remote(src, dst, send, recv, device):
        pltpu.make_async_remote_copy(
            src_ref=src, dst_ref=dst, send_sem=send, recv_sem=recv, device_id=device, device_id_type=MESH
        ).start()

    def settle(ref, sem):
        pltpu.make_async_copy(ref, ref, sem).wait()

    def rows_of(off, m):
        return pl.ds(pl.multiple_of(off, 16), m)

    off = [q * (length // streams) for q in range(streams)]
    span = [length // streams] * streams

    def start_reduce(q, ph):
        a = plans[q][ph]
        m = span[q] // size[a]
        for k in range(1, size[a]):
            p, dev = peer(a, k)
            src = w_ref.at[rows_of(off[q] + p * m, m)] if ph == 0 else held[q][ph - 1].at[rows_of(p * m, m)]
            remote(src, stage[q][ph].at[k - 1], w_send, w_recv.at[q, ph], dev)

    def finish_reduce(q, ph):
        a = plans[q][ph]
        g = size[a]
        m = span[q] // g
        if g > 1:
            settle(stage[q][ph], w_recv.at[q, ph])
        mine = rows_of(off[q] + at[a] * m, m) if ph == 0 else rows_of(at[a] * m, m)
        total = (w_ref[mine] if ph == 0 else held[q][ph - 1][mine]).astype(F32)
        for k in range(g - 1):
            total = total + stage[q][ph][k].astype(F32)
        off[q] = off[q] + at[a] * m
        span[q] = m
        if ph < len(plans[q]) - 1:
            held[q][ph][...] = total.astype(BF16)
        else:
            wout[core, rows_of(off[q], m)] = total.astype(BF16)

    def start_gather(q, ph):
        a = plans[q][ph]
        block = wout.at[core, rows_of(off[q], span[q])]
        for k in range(1, size[a]):
            remote(block, block, w_send, w_recv.at[q, 3 + ph], peer(a, k)[1])

    def send_across(row, m):
        block = wout.at[core, rows_of(row, m)]
        remote(block, block, c_send, c_recv, partner)

    def finish_gather(q, ph):
        a = plans[q][ph]
        if size[a] > 1:
            settle(stage[q][ph], w_recv.at[q, 3 + ph])
        off[q] = off[q] - at[a] * span[q]
        span[q] = span[q] * size[a]
        if ph == 1:
            send_across(off[q], span[q])
        if ph == 0:
            part = span[q] // size[a]
            for k in range(1, size[a]):
                send_across(off[q] + peer(a, k)[0] * part, part)

    def advance(q, st):
        if st < 3:
            finish_reduce(q, st)
            if st < 2:
                start_reduce(q, st + 1)
            else:
                start_gather(q, 2)
        else:
            finish_gather(q, 5 - st)
            if st < 5:
                start_gather(q, 4 - st)

    def start_sums(ph):
        a = "xyz"[ph]
        width = stride[a]
        block = pl.ds(me // width * width, width)
        for k in range(1, size[a]):
            remote(sout.at[block], sout.at[block], s_send, s_recv.at[ph], peer(a, k)[1])

    def finish_sums(ph):
        a = "xyz"[ph]
        if size[a] > 1:
            settle(sout.at[pl.ds(0, (size[a] - 1) * stride[a])], s_recv.at[ph])

    bout[core] = b_ref[...].astype(BF16)
    remote(bout.at[core], bout.at[core], b_send, b_recv, partner)
    ssum[...] = jnp.zeros_like(ssum)
    until = []
    for slots in zip(*SLOTS):
        ends = [sum(firsts[work[-1][0], work[-1][2] * t // LANES - 1][1:]) for work in slots]
        until.append(min(ends) * streams // length)
    until[-1] = streams
    table = timetable(streams, plans, size, 4 * LANES * length // streams, until)
    started = 0
    for slot in range(len(SLOTS[0])):
        for c in range(2):
            @pl.when(core == c)
            def _(slot=slot, c=c):
                work, at_col = [], 0
                for i, lo, hi in SLOTS[c][slot]:
                    work.append((i, lo * t, hi * t, at_col))
                    at_col += (hi - lo) * t
                acc[:, :at_col] = jnp.zeros((t, at_col), F32)
                reps = TILES if slot == 0 else 2
                deep = n // reps

                @pl.loop(0, reps)
                def _(step):
                    if slot == 0:
                        tile_copy(step).wait()
                    part = pl.ds(pl.multiple_of(step * deep, deep), deep)
                    if slot == 0:
                        ssum[...] += dot(jnp.ones((8, deep), BF16), e[part, :], 1, 0)
                    for i, lo, hi, col in work:
                        acc[:, col:col + hi - lo] += dot(e[part, i * t:(i + 1) * t], e[part, lo:hi], 0, 0)

                if slot == 0:
                    sums = ssum[0:1, :]
                    left[...] = stack(split3(sums * (1.0 / n)), (0, 0, 1, 1, 0, 2))
                    right[...] = stack(split3(sums), (0, 1, 0, 1, 2, 0))
                for i, lo, hi, col in work:
                    v = acc[:, col:col + hi - lo] - dot(left[:, i * t:(i + 1) * t], right[:, lo:hi], 0, 0)
                    v = v.astype(BF16)
                    for l in range(lo // LANES, hi // LANES):
                        _, first, m = firsts[i, l]
                        w_ref[first:first + m, :] = v[:m, l * LANES - lo:(l + 1) * LANES - lo]
                if slot == len(SLOTS[0]) - 1 and fill[c] < length:
                    w_ref[fill[c]:length, :] = jnp.zeros((length - fill[c], LANES), BF16)

        for q in range(started, until[slot]):
            start_reduce(q, 0)
        started = until[slot]
        if slot < len(SLOTS[0]) - 1:
            for st, q in table[slot]:
                advance(q, st)
        if slot == 0:
            sout[me] = ssum[0:1, :]
            start_sums(0)
        elif slot < 3:
            finish_sums(slot - 1)
            start_sums(slot)
    finish_sums(2)
    mean = jnp.sum(sout[:, 0, :], axis=0, keepdims=True) * (1.0 / (n * r))

    def make_unit(i):
        @pl.loop(0, n // UNITS // STEP)
        def _(step):
            at_rows = pl.ds(pl.multiple_of(i * (n // UNITS) + step * STEP, STEP), STEP)
            centered = e[at_rows, :].astype(F32) - mean
            e[at_rows, :] = (
                centered * lax.rsqrt(jnp.sum(centered * centered, axis=1, keepdims=True) + 1.0)
            ).astype(BF16)

        at_rows = pl.ds(i * (n // UNITS), n // UNITS)
        pltpu.make_async_copy(e.at[at_rows], u_hbm.at[at_rows], u_sem).start()

    units = 0
    for event in table[-1]:
        if event is None:
            make_unit(units)
            units += 1
        else:
            advance(event[1], event[0])
    settle(wout.at[0], c_recv)
    settle(wout.at[0], c_send)
    settle(bout.at[0], b_recv)
    settle(bout.at[0], b_send)
    settle(wout.at[:, pl.ds(0, length - length // r)], w_send)
    settle(sout.at[pl.ds(0, r - 1)], s_send)
    pltpu.make_async_copy(e, u_hbm, u_sem).wait()


def reduce(r, e, b):
    n, d = e.shape
    t = d // len(OWNER)
    length = packed_length(d, r)
    nz, ny, nx = factors(r)
    size = {"x": nx, "y": ny, "z": nz}
    streams = stream_count(length, r)
    stages, helds = [], []
    for plan in plans_of(streams):
        m = length // streams
        for ph, a in enumerate(plan):
            m //= size[a]
            stages.append(pltpu.VMEM((max(size[a] - 1, 1), m, LANES), BF16))
            if ph < 2:
                helds.append(pltpu.VMEM((m, LANES), BF16))
    vm = pl.BlockSpec(memory_space=pltpu.VMEM)
    hbm = pl.BlockSpec(memory_space=pltpu.HBM)
    dma = pltpu.SemaphoreType.DMA
    return pl.pallas_call(
        functools.partial(reduce_kernel, r),
        in_specs=[hbm, vm],
        out_specs=[vm] * 3 + [hbm],
        out_shape=[
            jax.ShapeDtypeStruct((2, length, LANES), BF16),
            jax.ShapeDtypeStruct((r, 1, d), F32),
            jax.ShapeDtypeStruct((2,) + b.shape, BF16),
            jax.ShapeDtypeStruct((n, d), BF16),
        ],
        scratch_shapes=[
            pltpu.VMEM((n, d), BF16),
            pltpu.VMEM((t, 3 * t), F32),
            pltpu.VMEM((8, d), F32),
            pltpu.VMEM((16, d), BF16),
            pltpu.VMEM((16, d), BF16),
            pltpu.VMEM((length, LANES), BF16),
            dma((TILES,)),
        ]
        + stages + helds + [dma((streams, 6)), dma((3,))] + [dma(())] * 7,
        compiler_params=pltpu.CompilerParams(collective_id=0, has_side_effects=True, vmem_limit_bytes=VMEM),
    )(e, b)


def shards(embeddings, start_basis):
    n, d = embeddings.shape
    r = lax.axis_size("rows")
    w, s, b, u = reduce(r, embeddings, start_basis)
    return finish(n, n * r, w, s, b, u)


def solution(mesh):
    in_specs = (P("rows", None), P(None, "cols"))
    out_specs = (P("rows", "cols"), P(None, "cols"))
    return jax.shard_map(shards, mesh=mesh, in_specs=in_specs, out_specs=out_specs, check_vma=False)
```

```python
import functools

import jax
import jax.numpy as jnp
from jax import lax
from jax.experimental import pallas as pl
from jax.experimental.pallas import tpu as pltpu
from jax.sharding import PartitionSpec as P

ITERS = 3
LANES = 128
MESH = pl.DeviceIdType.MESH
TILES = 4
NEAR = 1
VMEM = 32 << 20
HI = lax.Precision.HIGHEST
F32 = jnp.float32
BF16 = jnp.bfloat16


def dot(a, b, ca, cb, precision=None):
    return lax.dot_general(a, b, (((ca,), (cb,)), ((), ())), precision=precision, preferred_element_type=F32)


def split(v):
    hi = v.astype(BF16)
    return hi, (v - hi.astype(F32)).astype(BF16)


def inverse_factor(a_ref, spread, k):
    b = LANES
    m = b // 8
    sub = lax.broadcasted_iota(jnp.int32, (8, b), 0)
    lane = lax.broadcasted_iota(jnp.int32, (8, b), 1)
    wide_lane = lax.broadcasted_iota(jnp.int32, (b, k), 1)
    wide_sub = lax.broadcasted_iota(jnp.int32, (b, k), 0)
    for lo in range(0, k, b):
        hi = lo + b
        left = [a_ref[lo + 8 * t:lo + 8 * t + 8, lo:hi] for t in range(m)]
        right = [(lane == sub + 8 * t).astype(F32) for t in range(m)]
        for p in range(m):
            cols = {
                t: [jnp.broadcast_to(left[t][:, 8 * p + c:8 * p + c + 1], (8, b)) for c in range(8)]
                for t in range(p, m)
            }
            slot = 10 * (p % 2)
            for j in range(8):
                spread[slot + j] = cols[p][j]
            spread[slot + 8] = left[p]
            spread[slot + 9] = right[p]
            a = [[jnp.broadcast_to(spread[slot + j, i:i + 1, :], (8, b)) for j in range(i + 1)] for i in range(8)]
            low = [[jnp.broadcast_to(spread[slot + 8 + h, c:c + 1, :], (8, b)) for c in range(8)] for h in range(2)]
            close = range(p + 1, min(p + 1 + NEAR, m))
            inv, f = [], [[None] * 8 for _ in range(8)]
            for j in range(8):
                r = 1.0 / a[j][j]
                inv.append(r)
                for i in range(j + 1, 8):
                    f[i][j] = a[i][j] * r
                    for c in range(j + 1, i + 1):
                        a[i][c] = a[i][c] - f[i][j] * a[c][j]
                for h in range(2):
                    for i in range(j + 1, 8):
                        low[h][i] = low[h][i] - f[i][j] * low[h][j]
                for t in close:
                    z = cols[t][j] * r
                    left[t] = left[t] - z * low[0][j]
                    right[t] = right[t] - z * low[1][j]
                    for i in range(j + 1, 8):
                        cols[t][i] = cols[t][i] - f[i][j] * cols[t][j]
            if p + 1 + NEAR < m:
                solved = [[low[h][i] * inv[i] for i in range(8)] for h in range(2)]
                for h in range(2):
                    for i in range(6, -1, -1):
                        v = solved[h][i]
                        for c in range(7, i, -1):
                            v = v - f[c][i] * solved[h][c]
                        solved[h][i] = v
                for t in range(p + 1 + NEAR, m):
                    for h, part in enumerate((left, right)):
                        u = [cols[t][c] * solved[h][c] for c in range(8)]
                        part[t] = part[t] - (((u[7] + u[6]) + (u[5] + u[4])) + ((u[3] + u[2]) + (u[1] + u[0])))
            v, d = low[1][0], inv[0]
            for i in range(1, 8):
                v = jnp.where(sub == i, low[1][i], v)
                d = jnp.where(sub == i, inv[i], d)
            root = lax.rsqrt(d)
            root = root * (1.5 - 0.5 * d * root * root)
            right[p] = v * (d * root)
        factor = jnp.concatenate(right, axis=0)
        inside = (wide_lane >= lo) & (wide_lane < hi)
        strip = dot(factor, jnp.where(inside, (wide_lane - lo == wide_sub).astype(F32), a_ref[lo:hi, :]), 1, 0, HI)
        for r0 in range(hi, k, b):
            turned = dot(a_ref[r0:r0 + b, lo:hi], factor, 1, 1, HI)
            a_ref[r0:r0 + b, :] = jnp.where(inside, 0.0, a_ref[r0:r0 + b, :]) - dot(turned, strip, 1, 0, HI)
        a_ref[lo:hi, :] = strip


def finish_kernel(n, total, w_ref, s_ref, b_ref, u_hbm, o_hbm, basis_hbm,
                  w, basis, mean, mean_t, a, spread, unit, out, half, u_sem, o_sem, h_sem):
    core = lax.axis_index("cols")
    d, k = basis.shape
    h = k // 2
    rows = n // TILES

    def unit_copy(i):
        at = pl.ds(pl.multiple_of(i * rows, rows), rows)
        return pltpu.make_async_copy(u_hbm.at[at], unit.at[at], u_sem.at[i])

    for i in range(TILES):
        unit_copy(i).start()
    for (i, l), (c, first, m) in packing(d)[0].items():
        v = w_ref[c, first:first + m, :]
        row, col = i * (d // len(OWNER)), l * LANES
        w[row:row + m, col:col + LANES] = v
        if row + m > col:
            v, m = v[:m - LANES], m - LANES
        if m > 0:
            w[col:col + LANES, row:row + m] = v.T
    s = s_ref[:, 0, :]
    r = s.shape[0]
    m = s * (1.0 / n) - jnp.sum(s, axis=0, keepdims=True) * (1.0 / total)
    mh, ml = split(m)
    mean[:r] = mh
    mean[r:] = ml
    mean_t[...] = jnp.concatenate([mh.astype(F32), ml.astype(F32), mh.astype(F32)], axis=0).T.astype(BF16)
    basis[...] = jnp.concatenate([b_ref[0], b_ref[1]], axis=1)
    cut = d // 2

    @pl.loop(0, ITERS)
    def _(_):
        bf = basis[...]
        inner = dot(mean[...], bf, 1, 0)
        ih, il = split((inner[:r] + inner[r:]) * float(n))
        side = jnp.concatenate([ih, ih, il], axis=0)
        parts = []
        for g in range(2):
            at = slice(g * cut, (g + 1) * cut)
            parts.append(split(dot(w[at, :], bf, 1, 0) + dot(mean_t[at, :], side, 1, 0)))
        for corner in (LANES, k):
            hh, cross, ll = 0.0, 0.0, 0.0
            for ph, plo in parts:
                ph, plo = ph[:, :corner], plo[:, :corner]
                hh += dot(ph, ph, 0, 0)
                cross += dot(plo, ph, 0, 0)
                ll += dot(plo, plo, 0, 0)
            part = hh + (ll + (cross + cross.T))
            if corner < k:
                a[:corner, :corner] = part
            else:
                a[:LANES, LANES:] = part[:LANES, LANES:]
                a[LANES:, :] = part[LANES:, :]
        inverse_factor(a, spread, k)
        below = lax.broadcasted_iota(jnp.int32, (k, k), 0) >= lax.broadcasted_iota(jnp.int32, (k, k), 1)
        lh, ll = split(jnp.where(below, a[...], 0.0))
        for g, (ph, plo) in enumerate(parts):
            new = dot(ph, lh, 1, 1) + (dot(ph, ll, 1, 1) + dot(plo, lh, 1, 1))
            at = slice(g * cut, (g + 1) * cut)
            half[at, :] = jnp.where(core == 0, new[:, :h], new[:, h:])
            basis[at, :] = new.astype(BF16)

    half_copy = pltpu.make_async_copy(half, basis_hbm, h_sem)
    half_copy.start()

    def out_copy(i):
        at = pl.ds(pl.multiple_of(i * rows, rows), rows)
        return pltpu.make_async_copy(out.at[at], o_hbm.at[at], o_sem.at[i])

    @pl.loop(0, TILES)
    def _(i):
        unit_copy(i).wait()
        for g in range(2):
            at = pl.ds(pl.multiple_of(i * rows + g * (rows // 2), rows // 2), rows // 2)
            coords = dot(unit[at, :], basis[...], 1, 0)
            scale = lax.rsqrt(jnp.sum(coords * coords, axis=1, keepdims=True) * (1.0 / k) + 0.0001)
            out[at, :] = (jnp.where(core == 0, coords[:, :h], coords[:, h:]) * scale).astype(BF16)
        out_copy(i).start()

    half_copy.wait()
    for i in range(TILES):
        out_copy(i).wait()


def finish(n, total, w, s, b, u):
    d, h = b.shape[1], b.shape[2]
    k = 2 * h
    vm = pl.BlockSpec(memory_space=pltpu.VMEM)
    hbm = pl.BlockSpec(memory_space=pltpu.HBM)
    dma = pltpu.SemaphoreType.DMA
    return pl.pallas_call(
        functools.partial(finish_kernel, n, total),
        in_specs=[vm] * 3 + [hbm],
        out_specs=[hbm] * 2,
        out_shape=[jax.ShapeDtypeStruct((n, h), BF16), jax.ShapeDtypeStruct((d, h), F32)],
        scratch_shapes=[
            pltpu.VMEM((d, d), BF16),
            pltpu.VMEM((d, k), BF16),
            pltpu.VMEM((2 * s.shape[0], d), BF16),
            pltpu.VMEM((d, 3 * s.shape[0]), BF16),
            pltpu.VMEM((k, k), F32),
            pltpu.VMEM((20, 8, LANES), F32),
            pltpu.VMEM((n, d), BF16),
            pltpu.VMEM((n, h), BF16),
            pltpu.VMEM((d, h), F32),
            dma((TILES,)),
            dma((TILES,)),
            dma(()),
        ],
        compiler_params=pltpu.CompilerParams(vmem_limit_bytes=VMEM),
    )(w, s, b, u)


def factors(r):
    z = 4 if r % 4 == 0 else 1
    x = 1
    while x * x < r // z:
        x *= 2
    return z, r // z // x, x


def split3(v):
    hi, rest = split(v)
    rest = v - hi.astype(F32)
    mid = rest.astype(BF16).astype(F32)
    return hi.astype(F32), mid, (rest - mid).astype(BF16).astype(F32)


def stack(parts, order):
    pad = jnp.zeros((16 - len(order), parts[0].shape[1]), F32)
    return jnp.concatenate([parts[i] for i in order] + [pad], axis=0).astype(BF16)


OWNER = (0, 1, 0, 1, 1, 1)
SLOTS = (
    (((0, 0, 3),), ((0, 3, 6),), ((2, 2, 4),), ((2, 4, 6),)),
    (((1, 1, 4),), ((1, 4, 6),), ((3, 3, 6),), ((4, 4, 6), (5, 5, 6))),
)
UNITS = 12
STEP = 128


def packing(d):
    t = d // len(OWNER)
    firsts, fill = {}, [0, 0]
    for i, c in enumerate(OWNER):
        for l in range(i * t // LANES, d // LANES):
            m = min(t, (l + 1) * LANES - i * t)
            firsts[i, l] = (c, fill[c], m)
            fill[c] += m
    return firsts, fill


def packed_length(d, r):
    unit = 5 * 16 * r
    return -(-max(packing(d)[1]) // unit) * unit


def stream_count(length, r):
    return 10 if length % (160 * r) == 0 else 5


PLANS = ("xyz", "yxz", "xyz", "yxz", "zxy")
SLOT_US = (3.3, 1.2, 1.2, 1.4)
RATE = 87e3
FLIGHT_US = {"x": 3.0, "y": 3.0, "z": 4.0}
STEP_US = 0.2
UNIT_US = 0.5
SUM_EVENTS = (0, 5, 10)


def plans_of(streams):
    return [PLANS[q % len(PLANS)] for q in range(streams)]


def timetable(streams, plans, size, chunk, until):
    free = dict.fromkeys("xyz", 0.0)
    due, table = {}, []
    now, left = 0.0, UNITS

    def launch(q, st):
        plan = plans[q]
        ph = min(st, 5 - st)
        share = chunk
        for a in plan[:ph + 1]:
            share /= size[a]
        g = size[plan[ph]]
        free[plan[ph]] = max(now, free[plan[ph]]) + share * (g // 2) * (g - g // 2) / RATE
        due[q] = (free[plan[ph]] + FLIGHT_US[plan[ph]], q, st)

    def take(at):
        _, q, st = at
        del due[q]
        if st < 5:
            launch(q, st + 1)
        return st, q

    started = 0
    for cost, stop in zip(SLOT_US, until):
        now += cost
        for q in range(started, stop):
            launch(q, 0)
        started = stop
        step = []
        if stop < streams:
            for at in sorted(v for v in due.values() if v[0] <= now):
                now += STEP_US
                step.append(take(at))
        table.append(step)
    while due:
        at = min(due.values())
        if left and at[0] - now > 0.3 and len(table[-1]) > SUM_EVENTS[-1]:
            now += UNIT_US
            left -= 1
            table[-1].append(None)
        else:
            now = max(now, at[0]) + STEP_US
            table[-1].append(take(at))
    table[-1] += [None] * left
    return table


def reduce_kernel(r, e_hbm, b_ref, wout, sout, bout, u_hbm, e, acc, ssum, left, right, w_ref, e_sem, *scratch):
    nz, ny, nx = factors(r)
    n, d = e.shape
    t = d // len(OWNER)
    firsts, fill = packing(d)
    length = w_ref.shape[0]
    streams = stream_count(length, r)
    plans = plans_of(streams)
    size = {"x": nx, "y": ny, "z": nz}
    stride = {"x": 1, "y": nx, "z": nx * ny}
    scratch = list(scratch)
    stage = [[scratch.pop(0) for _ in plan] for plan in plans]
    held = [[scratch.pop(0) for _ in plan[:-1]] for plan in plans]
    w_recv, s_recv, w_send, s_send, c_send, c_recv, b_send, b_recv, u_sem = scratch

    me = lax.axis_index("rows")
    core = lax.axis_index("cols")
    tile = n // TILES

    def tile_copy(i):
        at_rows = pl.ds(pl.multiple_of(i * tile, tile), tile)
        return pltpu.make_async_copy(e_hbm.at[at_rows], e.at[at_rows], e_sem.at[i])

    for i in range(TILES):
        tile_copy(i).start()
    at = {a: lax.rem(me // stride[a], size[a]) for a in size}
    partner = {"cols": 1 - core}

    def peer(a, k):
        p = lax.rem(at[a] + k, size[a])
        return p, {"rows": me + (p - at[a]) * stride[a]}

    barrier = pltpu.get_barrier_semaphore()
    count = 1
    pl.semaphore_signal(barrier, inc=1, device_id=partner, device_id_type=MESH)
    for a in size:
        for k in range(1, size[a]):
            pl.semaphore_signal(barrier, inc=1, device_id=peer(a, k)[1], device_id_type=MESH)
            count += 1
    pl.semaphore_wait(barrier, count)

    def remote(src, dst, send, recv, device):
        pltpu.make_async_remote_copy(
            src_ref=src, dst_ref=dst, send_sem=send, recv_sem=recv, device_id=device, device_id_type=MESH
        ).start()

    def settle(ref, sem):
        pltpu.make_async_copy(ref, ref, sem).wait()

    def rows_of(off, m):
        return pl.ds(pl.multiple_of(off, 16), m)

    off = [q * (length // streams) for q in range(streams)]
    span = [length // streams] * streams

    def start_reduce(q, ph):
        a = plans[q][ph]
        m = span[q] // size[a]
        for k in range(1, size[a]):
            p, dev = peer(a, k)
            src = w_ref.at[rows_of(off[q] + p * m, m)] if ph == 0 else held[q][ph - 1].at[rows_of(p * m, m)]
            remote(src, stage[q][ph].at[k - 1], w_send, w_recv.at[q, ph], dev)

    def finish_reduce(q, ph):
        a = plans[q][ph]
        g = size[a]
        m = span[q] // g
        if g > 1:
            settle(stage[q][ph], w_recv.at[q, ph])
        mine = rows_of(off[q] + at[a] * m, m) if ph == 0 else rows_of(at[a] * m, m)
        total = (w_ref[mine] if ph == 0 else held[q][ph - 1][mine]).astype(F32)
        for k in range(g - 1):
            total = total + stage[q][ph][k].astype(F32)
        off[q] = off[q] + at[a] * m
        span[q] = m
        if ph < len(plans[q]) - 1:
            held[q][ph][...] = total.astype(BF16)
        else:
            wout[core, rows_of(off[q], m)] = total.astype(BF16)

    def start_gather(q, ph):
        a = plans[q][ph]
        block = wout.at[core, rows_of(off[q], span[q])]
        for k in range(1, size[a]):
            remote(block, block, w_send, w_recv.at[q, 3 + ph], peer(a, k)[1])

    def send_across(row, m):
        block = wout.at[core, rows_of(row, m)]
        remote(block, block, c_send, c_recv, partner)

    def finish_gather(q, ph):
        a = plans[q][ph]
        if size[a] > 1:
            settle(stage[q][ph], w_recv.at[q, 3 + ph])
        off[q] = off[q] - at[a] * span[q]
        span[q] = span[q] * size[a]
        if ph == 1:
            send_across(off[q], span[q])
        if ph == 0:
            part = span[q] // size[a]
            for k in range(1, size[a]):
                send_across(off[q] + peer(a, k)[0] * part, part)

    def advance(q, st):
        if st < 3:
            finish_reduce(q, st)
            if st < 2:
                start_reduce(q, st + 1)
            else:
                start_gather(q, 2)
        else:
            finish_gather(q, 5 - st)
            if st < 5:
                start_gather(q, 4 - st)

    def start_sums(ph):
        a = "xyz"[ph]
        width = stride[a]
        block = pl.ds(me // width * width, width)
        for k in range(1, size[a]):
            remote(sout.at[block], sout.at[block], s_send, s_recv.at[ph], peer(a, k)[1])

    def finish_sums(ph):
        a = "xyz"[ph]
        if size[a] > 1:
            settle(sout.at[pl.ds(0, (size[a] - 1) * stride[a])], s_recv.at[ph])

    bout[core] = b_ref[...].astype(BF16)
    remote(bout.at[core], bout.at[core], b_send, b_recv, partner)
    ssum[...] = jnp.zeros_like(ssum)
    until = []
    for slots in zip(*SLOTS):
        ends = [sum(firsts[work[-1][0], work[-1][2] * t // LANES - 1][1:]) for work in slots]
        until.append(min(ends) * streams // length)
    until[-1] = streams
    table = timetable(streams, plans, size, 4 * LANES * length // streams, until)
    started = 0
    for slot in range(len(SLOTS[0])):
        for c in range(2):
            @pl.when(core == c)
            def _(slot=slot, c=c):
                work, at_col = [], 0
                for i, lo, hi in SLOTS[c][slot]:
                    work.append((i, lo * t, hi * t, at_col))
                    at_col += (hi - lo) * t
                acc[:, :at_col] = jnp.zeros((t, at_col), F32)
                reps = TILES if slot == 0 else 2
                deep = n // reps

                @pl.loop(0, reps)
                def _(step):
                    if slot == 0:
                        tile_copy(step).wait()
                    part = pl.ds(pl.multiple_of(step * deep, deep), deep)
                    if slot == 0:
                        ssum[...] += dot(jnp.ones((8, deep), BF16), e[part, :], 1, 0)
                    for i, lo, hi, col in work:
                        acc[:, col:col + hi - lo] += dot(e[part, i * t:(i + 1) * t], e[part, lo:hi], 0, 0)

                if slot == 0:
                    sums = ssum[0:1, :]
                    left[...] = stack(split3(sums * (1.0 / n)), (0, 0, 1, 1, 0, 2))
                    right[...] = stack(split3(sums), (0, 1, 0, 1, 2, 0))
                for i, lo, hi, col in work:
                    v = acc[:, col:col + hi - lo] - dot(left[:, i * t:(i + 1) * t], right[:, lo:hi], 0, 0)
                    v = v.astype(BF16)
                    for l in range(lo // LANES, hi // LANES):
                        _, first, m = firsts[i, l]
                        w_ref[first:first + m, :] = v[:m, l * LANES - lo:(l + 1) * LANES - lo]
                if slot == len(SLOTS[0]) - 1 and fill[c] < length:
                    w_ref[fill[c]:length, :] = jnp.zeros((length - fill[c], LANES), BF16)

        for q in range(started, until[slot]):
            start_reduce(q, 0)
        started = until[slot]
        if slot < len(SLOTS[0]) - 1:
            for st, q in table[slot]:
                advance(q, st)
        if slot == 0:
            sout[me] = ssum[0:1, :]
            start_sums(0)

    def make_unit(i, mean):
        @pl.loop(0, n // UNITS // STEP)
        def _(step):
            at_rows = pl.ds(pl.multiple_of(i * (n // UNITS) + step * STEP, STEP), STEP)
            centered = e[at_rows, :].astype(F32) - mean
            e[at_rows, :] = (
                centered * lax.rsqrt(jnp.sum(centered * centered, axis=1, keepdims=True) + 1.0)
            ).astype(BF16)

        at_rows = pl.ds(i * (n // UNITS), n // UNITS)
        pltpu.make_async_copy(e.at[at_rows], u_hbm.at[at_rows], u_sem).start()

    units, count = 0, 0
    for event in table[-1]:
        if event is None:
            make_unit(units, mean)
            units += 1
            continue
        if count in SUM_EVENTS:
            ph = SUM_EVENTS.index(count)
            finish_sums(ph)
            if ph < 2:
                start_sums(ph + 1)
            else:
                fresh = jnp.sum(sout[:, 0, :], axis=0, keepdims=True)
                mean = fresh * (1.0 / (n * r))
        count += 1
        advance(event[1], event[0])
    settle(wout.at[0], c_recv)
    settle(wout.at[0], c_send)
    settle(bout.at[0], b_recv)
    settle(bout.at[0], b_send)
    settle(wout.at[:, pl.ds(0, length - length // r)], w_send)
    settle(sout.at[pl.ds(0, r - 1)], s_send)
    pltpu.make_async_copy(e, u_hbm, u_sem).wait()


def reduce(r, e, b):
    n, d = e.shape
    t = d // len(OWNER)
    length = packed_length(d, r)
    nz, ny, nx = factors(r)
    size = {"x": nx, "y": ny, "z": nz}
    streams = stream_count(length, r)
    stages, helds = [], []
    for plan in plans_of(streams):
        m = length // streams
        for ph, a in enumerate(plan):
            m //= size[a]
            stages.append(pltpu.VMEM((max(size[a] - 1, 1), m, LANES), BF16))
            if ph < 2:
                helds.append(pltpu.VMEM((m, LANES), BF16))
    vm = pl.BlockSpec(memory_space=pltpu.VMEM)
    hbm = pl.BlockSpec(memory_space=pltpu.HBM)
    dma = pltpu.SemaphoreType.DMA
    return pl.pallas_call(
        functools.partial(reduce_kernel, r),
        in_specs=[hbm, vm],
        out_specs=[vm] * 3 + [hbm],
        out_shape=[
            jax.ShapeDtypeStruct((2, length, LANES), BF16),
            jax.ShapeDtypeStruct((r, 1, d), F32),
            jax.ShapeDtypeStruct((2,) + b.shape, BF16),
            jax.ShapeDtypeStruct((n, d), BF16),
        ],
        scratch_shapes=[
            pltpu.VMEM((n, d), BF16),
            pltpu.VMEM((t, 3 * t), F32),
            pltpu.VMEM((8, d), F32),
            pltpu.VMEM((16, d), BF16),
            pltpu.VMEM((16, d), BF16),
            pltpu.VMEM((length, LANES), BF16),
            dma((TILES,)),
        ]
        + stages + helds + [dma((streams, 6)), dma((3,))] + [dma(())] * 7,
        compiler_params=pltpu.CompilerParams(collective_id=0, has_side_effects=True, vmem_limit_bytes=VMEM),
    )(e, b)


def shards(embeddings, start_basis):
    n, d = embeddings.shape
    r = lax.axis_size("rows")
    w, s, b, u = reduce(r, embeddings, start_basis)
    return finish(n, n * r, w, s, b, u)


def solution(mesh):
    in_specs = (P("rows", None), P(None, "cols"))
    out_specs = (P("rows", "cols"), P(None, "cols"))
    return jax.shard_map(shards, mesh=mesh, in_specs=in_specs, out_specs=out_specs, check_vma=False)
```
